768 devices in a mesh: tok: 12 (over x, z_lo), row: 2 (over core), col: 32 (over z_hi, y).
Axes of the slice: x: 4, y: 8, z: 12 (z_hi: 4, z_lo: 3; z = z_hi * 3 + z_lo), core: 2. Of those that a mesh axis runs over, the one named last changes fastest.
Arguments:
- activations: bfloat16 [6144, 4096], P(('tok', 'col'), 'row'), may hold values from -6 to 6
- grads_t: bfloat16 [12, 2464, 6144], P(None, 'col', ('tok', 'row')), may hold values from -0.14941406 to 0.14941406
Outputs:
- weight_grad: float32 [12, 2464, 4096], P('tok', 'col', 'row')
The draws below stay inside these ranges and needn't reach their ends.
All inputs are finite; a program needn't handle non-finite values.
Results may differ from the reference program's by a relative error of at most 0.0003.
Values may be sent and summed in bfloat16 or wider, within the bound.
No kernel may reach another device: no remote copies, remote signals or barrier semaphores. Data moves between devices by JAX's collectives and lax.ppermute only.
A program may use at most 32 MiB of HBM per device.

```python
import jax
import jax.numpy as jnp

D = 4096
FF = 29568
TOK_DEV = 512
TOKENS = 6144
N_TOK = 12


def raised(drawn, stream_key, source, target, shards_of, factor):
    def block_of(dim):
        return (jnp.arange(drawn.shape[dim]) // (drawn.shape[dim] // shards_of)).reshape((-1,) + (1,) * (drawn.ndim - 1 - dim))

    first = jax.random.permutation(stream_key, shards_of)[block_of(target)]
    second = (block_of(target) + shards_of // 2) % shards_of
    return jnp.where((block_of(source) == first) | (block_of(source) == second), factor * drawn, drawn)


def shard_levels(stream_key, extent, split, low, high):
    def one(dim, shards_of):
        draws = jax.random.uniform(jax.random.fold_in(jax.random.fold_in(stream_key, 6), dim), (shards_of,), jnp.float32, low / len(split), high / len(split))
        return jnp.repeat(jnp.exp(draws), extent[dim] // shards_of).reshape((-1,) + (1,) * (len(extent) - dim - 1))

    level = one(*split[0])
    for cut in split[1:]:
        level = level * one(*cut)
    return level


def noise(rng, dims, spread, bound, split=(), kind=jnp.bfloat16):
    factor_of = shard_levels(rng, dims, split, -0.22, 0.18) if split else 1.0
    entries = jax.random.normal(rng, dims, jnp.float32) * spread * factor_of
    return jnp.minimum(jnp.maximum(entries, -bound), bound).astype(kind)


def gaussian_with(rng, dims, spread, reach, shards, heavy, held_as=jnp.bfloat16):
    values = spread * jax.random.normal(rng, dims, jnp.float32)
    if shards:
        values = values * shard_levels(rng, dims, shards, -0.22, 0.18)
    return jnp.clip(raised(values, jax.random.fold_in(rng, 3), *heavy), -reach, reach).astype(held_as)


def setup_inputs(seed: int = 0) -> dict:
    splits = jax.random.split(jax.random.key(seed), 3)
    return {
        "activations": noise(splits[0], (TOKENS, D), 1.0, 6.0, ((0, 384), (1, 2))),
        "grads_t": gaussian_with(splits[1], (N_TOK, FF // N_TOK, TOKENS), 0.025, 0.14941406, ((1, 32), (2, 24)), (2, 0, 12, 2.0)),
    }


def reference(activations, grads_t):
    flat = grads_t.reshape(FF, TOKENS)
    total = jnp.zeros((FF, D), jnp.float32)
    for group in range(N_TOK):
        block = flat[:, group * TOK_DEV:(group + 1) * TOK_DEV]
        rows = activations[group * TOK_DEV:(group + 1) * TOK_DEV]
        total = total + jnp.dot(block, rows, preferred_element_type=jnp.float32)
    return total.reshape(N_TOK, FF // N_TOK, D)
```

```python
import jax
import jax.numpy as jnp
from jax import lax
from jax.experimental import pallas as pl
from jax.experimental.pallas import tpu as pltpu
from jax.sharding import Mesh
from jax.sharding import PartitionSpec as P


TOK = ("tok_0", "tok_1")


def exchange(blocks, axis):
    return lax.all_to_all(blocks, axis, 0, 0, tiled=True)


def shifted(array, axis, by):
    count = lax.axis_size(axis)
    return lax.ppermute(array, axis, [(k, (k + by) % count) for k in range(count)])


def round_the_ring(piece):
    count, place = lax.axis_size("col_1"), lax.axis_index("col_1")
    outer, own, width = piece.shape
    rows = jnp.zeros((outer, count, own, width), piece.dtype)

    def put(rows, block, source):
        return lax.dynamic_update_slice(rows, block[:, None], (0, source % count, 0, 0))

    rows = put(rows, piece, place)
    up = down = piece
    for step in range(1, count // 2):
        up, down = shifted(up, "col_1", 1), shifted(down, "col_1", -1)
        rows = put(put(rows, up, place - step + count), down, place + step)
    half = outer // 2
    last = jnp.concatenate([shifted(up[:half], "col_1", 1), shifted(down[half:], "col_1", -1)])
    rows = put(rows, last, place + count // 2)
    return rows.reshape(-1, width)


def product_kernel(side_ref, mine_ref, other_ref, rows_ref, out_ref, total_ref, *, units):
    blocks, _, depth = mine_ref.shape
    side = side_ref[0]
    for k in range(blocks):
        own = rows_ref[pl.ds(pl.multiple_of((2 * k + side) * depth, depth), depth), :]
        far = rows_ref[pl.ds(pl.multiple_of((2 * k + 1 - side) * depth, depth), depth), :]
        add = jnp.dot(mine_ref[k], own, preferred_element_type=jnp.float32)
        add += jnp.dot(other_ref[k], far, preferred_element_type=jnp.float32)
        if k == 0:
            total_ref[...] = add
        else:
            total_ref[...] += add
    limit = jnp.maximum(jnp.max(jnp.abs(total_ref[...])), 1e-30)
    exponent = jnp.ceil(jnp.log2(jnp.full((1, 128), limit, jnp.float32))) - 15.0
    exponent = jnp.max(exponent)
    scale = jnp.max(jnp.exp2(jnp.full((1, 128), -exponent, jnp.float32)))
    groups, padded, _ = out_ref.shape
    row = lax.broadcasted_iota(jnp.int32, out_ref.shape[1:], 0)
    for g in range(groups):
        values = total_ref[g * padded : (g + 1) * padded, :] * scale
        out_ref[g] = jnp.where(row < units, values, exponent)


def product(side, mine, other, rows, groups, units):
    _, height, _ = mine.shape
    width = rows.shape[1]
    return pl.pallas_call(
        lambda *refs: product_kernel(*refs, units=units),
        out_shape=jax.ShapeDtypeStruct((groups, height // groups, width), jnp.float32),
        in_specs=[
            pl.BlockSpec(memory_space=pltpu.SMEM),
            *(pl.BlockSpec(memory_space=pltpu.VMEM) for _ in range(3)),
        ],
        out_specs=pl.BlockSpec(memory_space=pltpu.VMEM),
        scratch_shapes=[pltpu.VMEM((height, width), jnp.float32)],
        compiler_params=pltpu.CompilerParams(vmem_limit_bytes=24 * 1024 * 1024),
        name="product",
    )(side, mine, other, rows)


def body(activations, grads_t):
    across, lower, outer = (lax.axis_size(name) for name in ("tok_0", "tok_1", "col_0"))
    groups, units, part = grads_t.shape
    own, width = activations.shape
    quarter = width // across
    padded = -(-units // 8) * 8 if units % 8 else units + 8

    quarters = activations.reshape(own, across, quarter).transpose(1, 0, 2)
    sent = jnp.broadcast_to(quarters[:, None], (across, outer, own, quarter)).reshape(-1, own, quarter)
    near = exchange(sent, ("tok_0", "col_0"))
    rows = round_the_ring(near)

    flat = jnp.pad(grads_t, ((0, 0), (0, padded - units), (0, 0))).reshape(groups * padded, part)
    mine = exchange(jnp.broadcast_to(flat[None], (across, *flat.shape)), "tok_0")
    other = shifted(mine, "row", 1)
    side = lax.axis_index("row").astype(jnp.int32)[None]
    partial = product(side, mine, other, rows, groups, units)
    received = exchange(partial.astype(jnp.float16), TOK)
    received = received.reshape(across, lower, padded, quarter)
    scale = jnp.exp2(received[:, :, units : units + 1, :1].astype(jnp.float32))
    sums = jnp.sum(received[:, :, :units].astype(jnp.float32) * scale, axis=1)
    return jnp.concatenate([sums[k] for k in range(across)], axis=-1)[None]


def solution(mesh):
    finer = Mesh(
        mesh.devices.reshape(4, 3, mesh.shape["row"], 4, 8),
        ("tok_0", "tok_1", "row", "col_0", "col_1"),
    )
    col, tok_col, tok_row = ("col_0", "col_1"), (*TOK, "col_0", "col_1"), (*TOK, "row")
    in_specs = (P(tok_col, "row"), P(None, col, tok_row))
    out_specs = P(TOK, col, "row")
    return jax.shard_map(body, mesh=finer, in_specs=in_specs, out_specs=out_specs, check_vma=False)
```

```python
import jax
import jax.numpy as jnp
from jax import lax
from jax.experimental import pallas as pl
from jax.experimental.pallas import tpu as pltpu
from jax.sharding import Mesh
from jax.sharding import PartitionSpec as P


TOK = ("tok_0", "tok_1")


def exchange(blocks, axis):
    return lax.all_to_all(blocks, axis, 0, 0, tiled=True)


def shifted(array, axis, by):
    count = lax.axis_size(axis)
    return lax.ppermute(array, axis, [(k, (k + by) % count) for k in range(count)])


def passed_on(array, by):
    count = lax.axis_size("col_1")
    steps = [(k, (k + by) % count) for k in range(count)]
    steps += [(count + k, count + (k - by) % count) for k in range(count)]
    return lax.ppermute(array, ("row", "col_1"), steps)


def round_the_ring(piece):
    count, place = lax.axis_size("col_1"), lax.axis_index("col_1")
    way = 1 - 2 * lax.axis_index("row")
    outer, own, width = piece.shape
    rows = jnp.zeros((outer, count, own, width), piece.dtype)

    def put(rows, block, source):
        return lax.dynamic_update_slice(rows, block[:, None], (0, (source + count) % count, 0, 0))

    rows = put(rows, piece, place)
    ahead1, back1 = passed_on(piece, 1), passed_on(piece, -1)
    ahead2, back2 = passed_on(piece, 2), passed_on(piece, -2)
    ahead3, back3 = passed_on(ahead2, 1), passed_on(back2, -1)
    ahead4 = passed_on(ahead2, 2)
    for step, block in ((1, ahead1), (-1, back1), (2, ahead2), (-2, back2), (3, ahead3), (4, ahead4), (-3, back3)):
        rows = put(rows, block, place - way * step)
    return rows.reshape(-1, width)


def product_kernel(place_ref, mine_ref, other_ref, rows_ref, out_ref, total_ref, *, units):
    blocks, _, depth = mine_ref.shape
    side, across = place_ref[0], place_ref[1]
    for k in range(blocks):
        first = 2 * lax.rem(across + blocks - k, blocks)
        own = rows_ref[pl.ds(pl.multiple_of((first + side) * depth, depth), depth), :]
        far = rows_ref[pl.ds(pl.multiple_of((first + 1 - side) * depth, depth), depth), :]
        add = jnp.dot(mine_ref[k], own, preferred_element_type=jnp.float32)
        add += jnp.dot(other_ref[k], far, preferred_element_type=jnp.float32)
        if k == 0:
            total_ref[...] = add
        else:
            total_ref[...] += add
    limit = jnp.maximum(jnp.max(jnp.abs(total_ref[...])), 1e-30)
    exponent = jnp.ceil(jnp.log2(jnp.full((1, 128), limit, jnp.float32))) - 15.0
    exponent = jnp.max(exponent)
    scale = jnp.max(jnp.exp2(jnp.full((1, 128), -exponent, jnp.float32)))
    groups, padded, _ = out_ref.shape
    row = lax.broadcasted_iota(jnp.int32, out_ref.shape[1:], 0)
    for g in range(groups):
        values = total_ref[g * padded : (g + 1) * padded, :] * scale
        out_ref[g] = jnp.where(row < units, values, exponent)


def product(place, mine, other, rows, groups, units):
    _, height, _ = mine.shape
    width = rows.shape[1]
    return pl.pallas_call(
        lambda *refs: product_kernel(*refs, units=units),
        out_shape=jax.ShapeDtypeStruct((groups, height // groups, width), jnp.float32),
        in_specs=[
            pl.BlockSpec(memory_space=pltpu.SMEM),
            *(pl.BlockSpec(memory_space=pltpu.VMEM) for _ in range(3)),
        ],
        out_specs=pl.BlockSpec(memory_space=pltpu.VMEM),
        scratch_shapes=[pltpu.VMEM((height, width), jnp.float32)],
        compiler_params=pltpu.CompilerParams(vmem_limit_bytes=24 * 1024 * 1024),
        name="product",
    )(place, mine, other, rows)


def body(activations, grads_t):
    across, lower, outer = (lax.axis_size(name) for name in ("tok_0", "tok_1", "col_0"))
    groups, units, held = grads_t.shape
    own, width = activations.shape
    quarter = width // across
    padded = -(-units // 8) * 8 if units % 8 else units + 8

    quarters = jnp.stack([activations[:, k * quarter : (k + 1) * quarter] for k in range(across)])
    sent = jnp.broadcast_to(quarters[:, None], (across, outer, own, quarter)).reshape(-1, own, quarter)
    near = exchange(sent, ("tok_0", "col_0"))
    rows = round_the_ring(near)

    flat = jnp.pad(grads_t, ((0, 0), (0, padded - units), (0, 0))).reshape(groups * padded, held)
    blocks = [flat, *(shifted(flat, "tok_0", k) for k in range(1, across))]
    mine = jnp.stack(blocks)
    other = shifted(mine, "row", 1)
    place = jnp.stack([lax.axis_index("row"), lax.axis_index("tok_0")]).astype(jnp.int32)
    partial = product(place, mine, other, rows, groups, units)
    received = exchange(partial.astype(jnp.float16), TOK)
    received = received.reshape(across, lower, padded, quarter)
    scale = jnp.exp2(received[:, :, units : units + 1, :1].astype(jnp.float32))
    sums = jnp.sum(received[:, :, :units].astype(jnp.float32) * scale, axis=1)
    return jnp.concatenate([sums[k] for k in range(across)], axis=-1)[None]


def solution(mesh):
    finer = Mesh(
        mesh.devices.reshape(4, 3, mesh.shape["row"], 4, 8),
        ("tok_0", "tok_1", "row", "col_0", "col_1"),
    )
    col, tok_col, tok_row = ("col_0", "col_1"), (*TOK, "col_0", "col_1"), (*TOK, "row")
    in_specs = (P(tok_col, "row"), P(None, col, tok_row))
    out_specs = P(TOK, col, "row")
    return jax.shard_map(body, mesh=finer, in_specs=in_specs, out_specs=out_specs, check_vma=False)
```

```python
import jax
import jax.numpy as jnp
from jax import lax
from jax.experimental import pallas as pl
from jax.experimental.pallas import tpu as pltpu
from jax.sharding import Mesh
from jax.sharding import PartitionSpec as P


TOK = ("tok_0", "tok_1")


def exchange(blocks, axis):
    return lax.all_to_all(blocks, axis, 0, 0, tiled=True)


def shifted(array, axis, by):
    count = lax.axis_size(axis)
    return lax.ppermute(array, axis, [(k, (k + by) % count) for k in range(count)])


def passed_on(array, by):
    count = lax.axis_size("col_1")
    steps = [(k, (k + by) % count) for k in range(count)]
    steps += [(count + k, count + (k - by) % count) for k in range(count)]
    return lax.ppermute(array, ("row", "col_1"), steps)


def round_the_ring(piece):
    count, place = lax.axis_size("col_1"), lax.axis_index("col_1")
    way = 1 - 2 * lax.axis_index("row")
    outer, own, width = piece.shape
    rows = jnp.zeros((outer, count, own, width), piece.dtype)

    def put(rows, block, source):
        return lax.dynamic_update_slice(rows, block[:, None], (0, (source + count) % count, 0, 0))

    rows = put(rows, piece, place)
    ahead1, back1 = passed_on(piece, 1), passed_on(piece, -1)
    ahead2, back2 = passed_on(piece, 2), passed_on(piece, -2)
    ahead3, back3 = passed_on(ahead2, 1), passed_on(back2, -1)
    ahead4 = passed_on(ahead2, 2)
    for step, block in ((1, ahead1), (-1, back1), (2, ahead2), (-2, back2), (3, ahead3), (4, ahead4), (-3, back3)):
        rows = put(rows, block, place - way * step)
    return rows.reshape(-1, width)


def product_kernel(place_ref, mine_ref, other_ref, rows_ref, out_ref, total_ref, *, units):
    blocks, height, depth = mine_ref.shape
    side, across = place_ref[0], place_ref[1]
    starts = []
    for k in range(blocks):
        first = 2 * lax.rem(across + blocks - k, blocks)
        starts.append([pl.multiple_of((first + half) * depth, depth) for half in (side, 1 - side)])
    tile = height // 4
    for m in range(4):
        part = slice(m * tile, (m + 1) * tile)
        add = None
        for k, (own, far) in enumerate(starts):
            for blocks_ref, start in ((mine_ref, own), (other_ref, far)):
                term = jnp.dot(blocks_ref[k, part], rows_ref[pl.ds(start, depth), :], preferred_element_type=jnp.float32)
                add = term if add is None else add + term
        total_ref[part, :] = add
    limit = jnp.maximum(jnp.max(jnp.abs(total_ref[...])), 1e-30)
    exponent = jnp.ceil(jnp.log2(jnp.full((1, 128), limit, jnp.float32))) - 15.0
    exponent = jnp.max(exponent)
    scale = jnp.max(jnp.exp2(jnp.full((1, 128), -exponent, jnp.float32)))
    groups, padded, _ = out_ref.shape
    row = lax.broadcasted_iota(jnp.int32, out_ref.shape[1:], 0)
    for g in range(groups):
        values = total_ref[g * padded : (g + 1) * padded, :] * scale
        out_ref[g] = jnp.where(row < units, values, exponent)


def product(place, mine, other, rows, groups, units):
    _, height, _ = mine.shape
    width = rows.shape[1]
    return pl.pallas_call(
        lambda *refs: product_kernel(*refs, units=units),
        out_shape=jax.ShapeDtypeStruct((groups, height // groups, width), jnp.float32),
        in_specs=[
            pl.BlockSpec(memory_space=pltpu.SMEM),
            *(pl.BlockSpec(memory_space=pltpu.VMEM) for _ in range(3)),
        ],
        out_specs=pl.BlockSpec(memory_space=pltpu.VMEM),
        scratch_shapes=[pltpu.VMEM((height, width), jnp.float32)],
        compiler_params=pltpu.CompilerParams(vmem_limit_bytes=24 * 1024 * 1024),
        name="product",
    )(place, mine, other, rows)


def body(activations, grads_t):
    across, lower, outer = (lax.axis_size(name) for name in ("tok_0", "tok_1", "col_0"))
    groups, units, held = grads_t.shape
    own, width = activations.shape
    quarter = width // across
    padded = -(-units // 8) * 8 if units % 8 else units + 8

    quarters = jnp.stack([activations[:, k * quarter : (k + 1) * quarter] for k in range(across)])
    sent = jnp.broadcast_to(quarters[:, None], (across, outer, own, quarter)).reshape(-1, own, quarter)
    near = exchange(sent, ("tok_0", "col_0"))
    rows = round_the_ring(near)

    flat = jnp.pad(grads_t, ((0, 0), (0, padded - units), (0, 0))).reshape(groups * padded, held)
    blocks = [flat, *(shifted(flat, "tok_0", k) for k in range(1, across))]
    mine = jnp.stack(blocks)
    other = shifted(mine, "row", 1)
    place = jnp.stack([lax.axis_index("row"), lax.axis_index("tok_0")]).astype(jnp.int32)
    partial = product(place, mine, other, rows, groups, units)
    received = exchange(partial.astype(jnp.float16), TOK)
    received = received.reshape(across, lower, padded, quarter)
    scale = jnp.exp2(received[:, :, units : units + 1, :1].astype(jnp.float32))
    sums = jnp.sum(received[:, :, :units].astype(jnp.float32) * scale, axis=1)
    return jnp.concatenate([sums[k] for k in range(across)], axis=-1)[None]


def solution(mesh):
    finer = Mesh(
        mesh.devices.reshape(4, 3, mesh.shape["row"], 4, 8),
        ("tok_0", "tok_1", "row", "col_0", "col_1"),
    )
    col, tok_col, tok_row = ("col_0", "col_1"), (*TOK, "col_0", "col_1"), (*TOK, "row")
    in_specs = (P(tok_col, "row"), P(None, col, tok_row))
    out_specs = P(TOK, col, "row")
    return jax.shard_map(body, mesh=finer, in_specs=in_specs, out_specs=out_specs, check_vma=False)
```
